256 devices in a mesh: seg: 4 (over y), tile: 64 (over z, x, core).
Axes of the slice: x: 4, y: 4, z: 8, core: 2. Of those that a mesh axis runs over, the one named last changes fastest.
Arguments:
- starting_warmth: float32 [2048, 65536], P('tile', 'seg'), may hold values from 0 to 1
- diffusivity_field: float32 [2048, 65536], P('tile', 'seg'), may hold values from 0.1 to 1
- emitter_mask: int32 [2048, 65536], P('tile', 'seg'), may hold values 0 or 1
Outputs:
- final_warmth: float32 [2048, 65536], P('tile', 'seg')
The draws below stay inside these ranges and needn't reach their ends.
Inputs may be any that keep to these rules, and one draw needn't show every extreme that they name: `emitter_mask`: nonzero marks a source vertex.
All inputs are finite; a program needn't handle non-finite values. No bound on the sum of `emitter_mask` on one device may be relied on, other than what follows from the above.
Results may differ from the reference program's by a relative error of at most 0.00002.
Values sent between devices are 32-bit elements; how exact they have to be, the bound alone decides.
A program may use at most 128 MiB of HBM per device.

```python
import math
import jax
import jax.numpy as jnp

STEPS = 8
BAND_BREADTH = 2048
BAND_EXTENT = 65536


def with_ends(values, rng, smallest, high):
    dims = values.shape
    index_at = [jax.random.randint(jax.random.fold_in(rng, axis), (), 0, dims[axis]) for axis in range(len(dims))]
    values = values.at[tuple(index_at)].set(smallest)
    longest = dims.index(max(dims))
    index_at[longest] = (index_at[longest] + 1) % dims[longest]
    return values.at[tuple(index_at)].set(high)


def block_scale(stream_key, shape, cuts, smallest, high):
    def one(axis_at, blocks):
        draws = jax.random.uniform(jax.random.fold_in(jax.random.fold_in(stream_key, 6), axis_at), (blocks,), jnp.float32, smallest / len(cuts), high / len(cuts))
        return jnp.repeat(jnp.exp(draws), shape[axis_at] // blocks).reshape((-1,) + (1,) * (len(shape) - axis_at - 1))

    loudness = one(*cuts[0])
    for cut in cuts[1:]:
        loudness = loudness * one(*cut)
    return loudness


def setup_inputs(seed: int = 0) -> dict:
    streams_of = jax.random.split(jax.random.key(seed), 4)
    return {
        "starting_warmth": jnp.clip(1.0 * jax.random.uniform(streams_of[0], (BAND_BREADTH, BAND_EXTENT), jnp.float32) ** block_scale(streams_of[0], (BAND_BREADTH, BAND_EXTENT), ((0, 64), (1, 4)), -0.2, 0.2), 0.0, 1.0),
        "diffusivity_field": jnp.clip(jnp.exp(math.log(1.0) - 2.3025851 * jax.random.uniform(streams_of[1], (BAND_BREADTH, BAND_EXTENT), jnp.float32) ** block_scale(streams_of[1], (BAND_BREADTH, BAND_EXTENT), ((0, 64), (1, 4)), -0.2, 0.2)), 0.1, 1.0),
        "emitter_mask": with_ends((jax.random.randint(streams_of[2], (BAND_BREADTH, BAND_EXTENT), 0, 64) < 1).astype(jnp.int32), jax.random.fold_in(streams_of[2], 1), 0, 1),
    }


time_step = 0.24


def advance(bordered_grid, conduct, source, interior_region):
    height = bordered_grid.shape[0] - 2
    length = bordered_grid.shape[1] - 2
    middle_point = bordered_grid[1:-1, 1:-1]
    self_conductance = conduct[1:-1, 1:-1]
    flux_sum = jnp.zeros_like(middle_point)
    for row_off, col_off in ((0, 1), (2, 1), (1, 0), (1, 2)):
        adjacent_cell = bordered_grid[row_off:row_off + height, col_off:col_off + length]
        near_conduct = conduct[row_off:row_off + height, col_off:col_off + length]
        flux_sum = flux_sum + 0.5 * (self_conductance + near_conduct) * (adjacent_cell - middle_point)
    updated = middle_point + time_step * flux_sum
    updated = jnp.where(source, jnp.float32(1.0), updated)
    if interior_region is not None:
        updated = updated * interior_region
    return updated


def reference(starting_warmth, diffusivity_field, emitter_mask):
    is_source = emitter_mask != 0
    conduct = jnp.pad(diffusivity_field, 1)
    present_warmth = starting_warmth
    for substep in range(STEPS):
        present_warmth = advance(jnp.pad(present_warmth, 1), conduct, is_source, None)
    return present_warmth
```

```python
import functools

import jax
import jax.numpy as jnp
from jax import lax
from jax.experimental import pallas as pl
from jax.experimental.pallas import tpu as pltpu
from jax.sharding import PartitionSpec as P

STEPS = 8
FACE = 0.24 * 0.5
ROWS = 32
GHOST = 4
NV = 16
MESH = pl.DeviceIdType.MESH

LINES = ((1, 1), (2, 1), (2, 2), (3, 2), (3, 3), (4, 3), (4, 4))


def at(row):
    return row + GHOST


def shift_east(row, lane):
    turned = [pltpu.roll(x, 127, 1) for x in row]
    turned.append(pltpu.roll(turned[0], 7, 0))
    return [jnp.where(lane == 127, turned[v + 1], turned[v]) for v in range(NV)]


def shift_west(row, lane):
    turned = [pltpu.roll(x, 1, 1) for x in row]
    before = [pltpu.roll(turned[-1], 1, 0)] + turned[:-1]
    return [jnp.where(lane == 0, before[v], turned[v]) for v in range(NV)]


def load(ref, row):
    return [ref[v, row] for v in range(NV)]


def kernel(
    f_in, c_in, m_in, out,
    heat, cond, mask, east, south, keep,
    edge_fc, edge_m, edge_out,
    load_sem, edge_load_sem, send_sem, recv_sem, side_send, side_recv, out_sem,
):
    tile = lax.axis_index("tile")
    seg = lax.axis_index("seg")
    n_tile = lax.axis_size("tile")
    n_seg = lax.axis_size("seg")
    has_up = tile > 0
    has_down = tile < n_tile - 1
    has_west = seg > 0
    has_east = seg < n_seg - 1
    lane = lax.broadcasted_iota(jnp.int32, (8, 128), 1)

    def edge_loads():
        copies = []
        for piece, (s, v) in enumerate(((0, 0), (7, 15))):
            for k, src in enumerate((f_in, c_in)):
                copies.append(pltpu.make_async_copy(
                    src.at[:, s, v], edge_fc.at[piece, k, pl.ds(1, 4)],
                    edge_load_sem.at[3 * piece + k]))
            copies.append(pltpu.make_async_copy(
                m_in.at[:, s, v], edge_m.at[piece, pl.ds(1, 4)],
                edge_load_sem.at[3 * piece + 2]))
        return copies

    arrays = ((f_in, heat.at[0]), (c_in, cond), (m_in, mask))

    def block_load(k, block):
        src, dst = arrays[k]
        for s in range(8):
            pltpu.make_async_copy(
                src.at[block, s], dst.at[:, pl.ds(at(8 * block), 8), s, :],
                load_sem.at[k, block]).start()

    def block_wait(k, block):
        dst = arrays[k][1].at[:, pl.ds(at(8 * block), 8)]
        pltpu.make_async_copy(dst, dst, load_sem.at[k, block]).wait()

    for block in (0, 3):
        for k in (0, 1):
            block_load(k, block)
    for copy in edge_loads():
        copy.start()
    for block in (0, 3):
        block_load(2, block)
    for block in (1, 2):
        for k in (1, 0, 2):
            block_load(k, block)

    barrier = pltpu.get_barrier_semaphore()
    sides = (
        (has_up, {"tile": tile - 1}), (has_down, {"tile": tile + 1}),
        (has_west, {"seg": seg - 1}), (has_east, {"seg": seg + 1}),
    )
    for there, device in sides:
        @pl.when(there)
        def _():
            pl.semaphore_signal(barrier, inc=1, device_id=device, device_id_type=MESH)
    count = sum(there.astype(jnp.int32) for there, _ in sides)
    pl.semaphore_wait(barrier, count)

    def rows_of(direction, near, far):
        if direction == 0:
            return near - 1, ROWS + near - 1, far - near + 1
        return ROWS - far, -far, far - near + 1

    def remote(direction, slot, src, dst):
        device = {"tile": tile - 1 if direction == 0 else tile + 1}
        return pltpu.make_async_remote_copy(
            src_ref=src, dst_ref=dst,
            send_sem=send_sem.at[direction, slot], recv_sem=recv_sem.at[direction, slot],
            device_id=device, device_id_type=MESH)

    def tile_copy(direction, slot):
        if slot == 0:
            ref, near, far = heat.at[0], 1, 1
        elif slot == 1:
            ref, near, far = cond, 1, 1
        elif slot == 2:
            ref, near, far = cond, 2, 4
        elif slot == 3:
            ref, near, far = mask, 1, 3
        elif slot < 6:
            block = 1 if direction == 0 else 4
            land = 5 if direction == 0 else 0
            if slot == 4:
                return remote(direction, slot, edge_fc.at[:, :, block], edge_fc.at[:, :, land])
            return remote(direction, slot, edge_m.at[:, block], edge_m.at[:, land])
        else:
            distance, time = LINES[slot - 6]
            ref, near, far = heat.at[time % 2], distance, distance
        src, dst, count = rows_of(direction, near, far)
        return remote(direction, slot, ref.at[:, pl.ds(at(src), count)],
                      ref.at[:, pl.ds(at(dst), count)])

    def send(slot):
        for direction, there in ((0, has_up), (1, has_down)):
            @pl.when(there)
            def _():
                tile_copy(direction, slot).start()

    def sent(slot):
        for direction, there in ((0, has_up), (1, has_down)):
            @pl.when(there)
            def _():
                tile_copy(direction, slot).wait_send()

    def received(slot):
        for direction, there in ((0, has_down), (1, has_up)):
            @pl.when(there)
            def _():
                tile_copy(direction, slot).wait_recv()

    def side_copy(direction, kind):
        device = {"seg": seg - 1 if direction == 0 else seg + 1}
        ref = edge_m if kind else edge_fc
        if kind:
            src, dst = ref.at[direction, pl.ds(1, 4)], ref.at[direction + 2, pl.ds(1, 4)]
        else:
            src, dst = ref.at[direction, :, pl.ds(1, 4)], ref.at[direction + 2, :, pl.ds(1, 4)]
        return pltpu.make_async_remote_copy(
            src_ref=src, dst_ref=dst,
            send_sem=side_send.at[direction, kind], recv_sem=side_recv.at[direction, kind],
            device_id=device, device_id_type=MESH)

    for block in (0, 3):
        for k in (0, 1):
            block_wait(k, block)
    send(0)
    send(1)
    for copy in edge_loads():
        copy.wait()
    for direction, there in ((0, has_west), (1, has_east)):
        @pl.when(there)
        def _():
            side_copy(direction, 0).start()
            side_copy(direction, 1).start()
    for block in (0, 3):
        block_wait(2, block)
    send(2)
    send(3)

    zero = jnp.zeros((8, 128), jnp.float32)
    for there, first in ((has_up, -GHOST), (has_down, ROWS)):
        @pl.when(jnp.logical_not(there))
        def _():
            @pl.loop(0, GHOST)
            def _(i):
                for v in range(NV):
                    for ref in (heat.at[0], heat.at[1], cond, keep):
                        ref[v, at(first) + i] = zero

    def east_row(row):
        c = load(cond, row)
        ce = shift_east(c, lane)
        for v in range(NV):
            east[v, row] = FACE * (c[v] + ce[v])

    def south_row(row):
        for v in range(NV):
            south[v, row] = FACE * (cond[v, row] + cond[v, row + 1])

    def keep_row(row):
        for v in range(NV):
            keep[v, row] = jnp.where(mask[v, row] != 0, 0.0, 1.0)

    for block in (1, 2):
        for k in range(3):
            block_wait(k, block)

    @pl.loop(0, ROWS // 4)
    def _(i):
        for j in range(4):
            row = at(0) + 4 * i + j
            east_row(row)
            keep_row(row)

    @pl.loop(0, ROWS // 4)
    def _(i):
        for j in range(4):
            south_row(at(0) + jnp.minimum(4 * i + j, ROWS - 2))

    def rows_step(time, rows, first=False):
        old, new = heat.at[(time - 1) % 2], heat.at[time % 2]
        above = load(old, rows[0] - 1)
        here = load(old, rows[0])
        north = [south[v, rows[0] - 1] * (here[v] - above[v]) for v in range(NV)]
        for row in rows:
            below = load(old, row + 1)
            down = [south[v, row] * (below[v] - here[v]) for v in range(NV)]
            ahead = shift_east(here, lane)
            flow = [east[v, row] * (ahead[v] - here[v]) for v in range(NV)]
            behind = shift_west(flow, lane)
            for v in range(NV):
                change = (flow[v] - behind[v]) + (down[v] - north[v])
                if first:
                    new[v, row] = jnp.where(mask[v, row] != 0, 1.0, here[v] + change)
                else:
                    new[v, row] = here[v] + keep[v, row] * change
            here, north = below, down

    def sweep(time, low, high, width, first=False):
        count = -(-(high - low) // width)

        @pl.loop(0, count)
        def _(i):
            start = at(jnp.minimum(low + i * width, high - width))
            rows_step(time, [start + j for j in range(width)], first)

    sweep(1, 1, ROWS - 1, 6, first=True)

    for direction, there in ((0, has_east), (1, has_west)):
        @pl.when(there)
        def _():
            side_copy(direction, 0).wait_recv()
            side_copy(direction, 1).wait_recv()
    received(0)
    received(1)
    south_row(at(-1))
    south_row(at(ROWS - 1))
    rows_step(1, [at(0)], first=True)
    rows_step(1, [at(ROWS - 1)], first=True)
    send(6)
    send(7)
    send(4)
    send(5)

    for time in range(2, STEPS + 1):
        level = time - 1
        sweep(time, level, ROWS - level, 6)
        for slot, (_, when) in enumerate(LINES):
            if when == time:
                send(6 + slot)

    received(4)
    received(5)
    shape = (48, 128)
    lane48 = lax.broadcasted_iota(jnp.int32, shape, 1)
    row48 = lax.broadcasted_iota(jnp.int32, shape, 0)
    first_row = jnp.where(has_up, 0, 8)
    end_row = jnp.where(has_down, 48, 40)
    for side in range(2):
        right, left = ((0, 3), (2, 1))[side]
        is_right = lane48 < 64
        first_lane = 0 if side == 0 else jnp.where(has_east, 0, 64)
        end_lane = jnp.where(has_west, 128, 64) if side == 0 else 128
        exists = ((row48 >= first_row) & (row48 < end_row)
                  & (lane48 >= first_lane) & (lane48 < end_lane))

        def pick(k):
            value = jnp.where(is_right, edge_fc[right, k].reshape(shape),
                              edge_fc[left, k].reshape(shape))
            return jnp.where(exists, value, 0.0)

        f = pick(0)
        c = pick(1)
        source = jnp.where(is_right, edge_m[right].reshape(shape),
                           edge_m[left].reshape(shape)) != 0
        source = jnp.logical_and(source, exists)
        stay = jnp.where(jnp.logical_and(exists, jnp.logical_not(source)), 1.0, 0.0)
        turns = ((127, 1), (1, 1), (47, 0), (1, 0))
        faces = [stay * (FACE * (c + pltpu.roll(c, *turn))) for turn in turns]

        def substep(f):
            total = f
            for turn, face in zip(turns, faces):
                total = total + face * (pltpu.roll(f, *turn) - f)
            return total

        f = jnp.where(source, 1.0, substep(f))
        f = lax.fori_loop(1, STEPS, lambda _, x: substep(x), f)
        edge_out[side] = f[8:40]

    received(2)
    received(3)
    for there, rows in ((has_up, (-3, -2, -1)), (has_down, (ROWS, ROWS + 1, ROWS + 2))):
        for row in rows:
            east_row(at(row))

        @pl.when(there)
        def _():
            for row in rows:
                keep_row(at(row))
    for row in (-4, -3, -2, ROWS, ROWS + 1, ROWS + 2):
        south_row(at(row))

    for slot in range(13):
        sent(slot)
    for slot in range(6, 13):
        received(slot)
    for time in range(2, STEPS + 1):
        level = time - 1
        out_by = min(level, 7 - level)
        top = [at(row) for row in range(-out_by, level)]
        bottom = [at(row) for row in range(ROWS - level, ROWS + out_by)]
        rows_step(time, top)
        rows_step(time, bottom)

    sub = lax.broadcasted_iota(jnp.int32, (8, 128), 0)
    final = heat.at[STEPS % 2]
    first_columns = jnp.logical_and(sub == 0, lane < 8)
    last_columns = jnp.logical_and(sub == 7, lane >= 120)

    @pl.loop(0, ROWS // 8)
    def _(i):
        for j in range(8):
            row = 8 * i + j
            for side, v, where in ((0, 0, first_columns), (1, NV - 1, last_columns)):
                patch = jnp.broadcast_to(edge_out[side, pl.ds(row, 1), :], (8, 128))
                final[v, at(row)] = jnp.where(where, patch, final[v, at(row)])

    def store(block, s):
        return pltpu.make_async_copy(
            final.at[:, pl.ds(at(8 * block), 8), s, :], out.at[block, s], out_sem.at[block, s])

    for block in range(4):
        for s in range(8):
            store(block, s).start()
    for block in range(4):
        for s in range(8):
            store(block, s).wait()
    for direction, there in ((0, has_west), (1, has_east)):
        @pl.when(there)
        def _():
            side_copy(direction, 0).wait_send()
            side_copy(direction, 1).wait_send()


def tiles(x):
    return x.reshape(4, 8, 8, NV, 128).transpose(0, 2, 3, 1, 4)


def shards(starting_warmth, diffusivity_field, emitter_mask):
    wide = ROWS + 2 * GHOST
    result = pl.pallas_call(
        kernel,
        out_shape=jax.ShapeDtypeStruct((4, 8, NV, 8, 128), jnp.float32),
        in_specs=[pl.BlockSpec(memory_space=pl.ANY)] * 3,
        out_specs=pl.BlockSpec(memory_space=pl.ANY),
        scratch_shapes=[
            pltpu.VMEM((2, NV, wide, 8, 128), jnp.float32),
            pltpu.VMEM((NV, wide, 8, 128), jnp.float32),
            pltpu.VMEM((NV, wide, 8, 128), jnp.int32),
            pltpu.VMEM((NV, wide, 8, 128), jnp.float32),
            pltpu.VMEM((NV, wide, 8, 128), jnp.float32),
            pltpu.VMEM((NV, wide, 8, 128), jnp.float32),
            pltpu.VMEM((4, 2, 6, 8, 128), jnp.float32),
            pltpu.VMEM((4, 6, 8, 128), jnp.int32),
            pltpu.VMEM((2, ROWS, 128), jnp.float32),
            pltpu.SemaphoreType.DMA((3, 4)),
            pltpu.SemaphoreType.DMA((6,)),
            pltpu.SemaphoreType.DMA((2, 13)),
            pltpu.SemaphoreType.DMA((2, 13)),
            pltpu.SemaphoreType.DMA((2, 2)),
            pltpu.SemaphoreType.DMA((2, 2)),
            pltpu.SemaphoreType.DMA((4, 8)),
        ],
        compiler_params=pltpu.CompilerParams(
            collective_id=0, has_side_effects=True, vmem_limit_bytes=60 * 2**20),
    )(tiles(starting_warmth), tiles(diffusivity_field), tiles(emitter_mask))
    return result.transpose(0, 3, 1, 2, 4).reshape(ROWS, 128 * 128)


def solution(mesh):
    return jax.shard_map(
        shards,
        mesh=mesh,
        in_specs=(P("tile", "seg"),) * 3,
        out_specs=P("tile", "seg"),
        check_vma=False,
    )
```

```python
import functools

import jax
import jax.numpy as jnp
from jax import lax
from jax.experimental import pallas as pl
from jax.experimental.pallas import tpu as pltpu
from jax.sharding import PartitionSpec as P

STEPS = 8
FACE = 0.24 * 0.5
ROWS = 32
GHOST = 4
NV = 16
LOW, HIGH = 7, 25
MESH = pl.DeviceIdType.MESH

LINES = ((1, 1), (2, 1), (2, 2), (3, 2), (3, 3), (4, 3), (4, 4))


def at(row):
    return row + GHOST


def reg(v):
    return pl.ds(8 * v, 8)


def load(ref, row):
    return [ref[row, reg(v), :] for v in range(NV)]


def position():
    return (lax.broadcasted_iota(jnp.int32, (8, 128), 0),
            lax.broadcasted_iota(jnp.int32, (8, 128), 1))


def after_last(first):
    sub, _ = position()
    down = pltpu.roll(first, 7, 0)
    return jnp.where(sub == 7, pltpu.roll(down, 127, 1), down)


def before_first(last):
    sub, _ = position()
    up = pltpu.roll(last, 1, 0)
    return jnp.where(sub == 0, pltpu.roll(up, 1, 1), up)


def comb(j):
    return pl.ds(64 * (j % 2) + j // 2, 8, stride=8)


def spread(x, ref, row):
    turned = x.T
    for j in range(NV):
        ref[row, comb(j), :] = turned[8 * j:8 * j + 8]


def gather(ref, row):
    return jnp.concatenate([ref[row, comb(j), :] for j in range(NV)], axis=0).T


def finish(ref, at_row, edge, row, put):
    sub, lane = position()
    x = gather(ref, at_row)
    for side, first, where in ((0, 0, (sub == 0) & (lane < 8)),
                               (1, 120, (sub == 7) & (lane >= 120))):
        patch = jnp.broadcast_to(edge[side, pl.ds(row, 1), :], (8, 128))
        put(pl.ds(first, 8), jnp.where(where, patch, x[first:first + 8]))
    put(pl.ds(8, 112), x[8:120])


def kernel(
    f_in, c_in, m_in,
    ready, border, edge_out,
    f_rows, c_rows, m_rows, heat, cond, east, west, south, keep,
    edge_fc, edge_m,
    load_sem, edge_load_sem, send_sem, recv_sem, side_send, side_recv,
):
    tile = lax.axis_index("tile")
    seg = lax.axis_index("seg")
    n_tile = lax.axis_size("tile")
    n_seg = lax.axis_size("seg")
    has_up = tile > 0
    has_down = tile < n_tile - 1
    has_west = seg > 0
    has_east = seg < n_seg - 1

    def edge_loads():
        copies = []
        for piece, block in enumerate((0, 127)):
            for k, src in enumerate((f_in, c_in)):
                copies.append(pltpu.make_async_copy(
                    src.at[:, block], edge_fc.at[piece, k, pl.ds(1, 4)],
                    edge_load_sem.at[3 * piece + k]))
            copies.append(pltpu.make_async_copy(
                m_in.at[:, block], edge_m.at[piece, pl.ds(1, 4)],
                edge_load_sem.at[3 * piece + 2]))
        return copies

    arrays = ((f_in, f_rows), (c_in, c_rows), (m_in, m_rows))
    groups = ((0, 31), (1, 2, 3, 28, 29, 30), tuple(range(4, 28)))

    def start_loads(k, group):
        src, dst = arrays[k]
        for row in groups[group]:
            pltpu.make_async_copy(
                src.at[row // 8, :, row % 8], dst.at[row], load_sem.at[k, group]).start()

    def wait_loads(k, group):
        dst = arrays[k][1].at[pl.ds(0, len(groups[group]))]
        pltpu.make_async_copy(dst, dst, load_sem.at[k, group]).wait()

    for k in range(3):
        start_loads(k, 0)
    for copy in edge_loads():
        copy.start()
    for group in (1, 2):
        for k in (1, 2, 0):
            start_loads(k, group)

    barrier = pltpu.get_barrier_semaphore()
    sides = (
        (has_up, {"tile": tile - 1}), (has_down, {"tile": tile + 1}),
        (has_west, {"seg": seg - 1}), (has_east, {"seg": seg + 1}),
    )
    for there, device in sides:
        @pl.when(there)
        def _():
            pl.semaphore_signal(barrier, inc=1, device_id=device, device_id_type=MESH)
    count = sum(there.astype(jnp.int32) for there, _ in sides)
    pl.semaphore_wait(barrier, count)

    def rows_of(direction, near, far):
        if direction == 0:
            return near - 1, ROWS + near - 1, far - near + 1
        return ROWS - far, -far, far - near + 1

    def remote(direction, slot, src, dst):
        device = {"tile": tile - 1 if direction == 0 else tile + 1}
        return pltpu.make_async_remote_copy(
            src_ref=src, dst_ref=dst,
            send_sem=send_sem.at[direction, slot], recv_sem=recv_sem.at[direction, slot],
            device_id=device, device_id_type=MESH)

    def tile_copy(direction, slot):
        if slot == 0:
            ref, near, far = heat.at[0], 1, 1
        elif slot == 1:
            ref, near, far = cond, 1, 1
        elif slot == 2:
            ref, near, far = cond, 2, 4
        elif slot == 3:
            ref, near, far = keep, 1, 3
        elif slot < 6:
            block = 1 if direction == 0 else 4
            land = 5 if direction == 0 else 0
            if slot == 4:
                return remote(direction, slot, edge_fc.at[:, :, block], edge_fc.at[:, :, land])
            return remote(direction, slot, edge_m.at[:, block], edge_m.at[:, land])
        else:
            distance, time = LINES[slot - 6]
            ref, near, far = heat.at[time % 2], distance, distance
        src, dst, count = rows_of(direction, near, far)
        return remote(direction, slot, ref.at[pl.ds(at(src), count)],
                      ref.at[pl.ds(at(dst), count)])

    def send(slot):
        for direction, there in ((0, has_up), (1, has_down)):
            @pl.when(there)
            def _():
                tile_copy(direction, slot).start()

    def sent(slot):
        for direction, there in ((0, has_up), (1, has_down)):
            @pl.when(there)
            def _():
                tile_copy(direction, slot).wait_send()

    def received(slot):
        for direction, there in ((0, has_down), (1, has_up)):
            @pl.when(there)
            def _():
                tile_copy(direction, slot).wait_recv()

    def side_copy(direction, kind):
        device = {"seg": seg - 1 if direction == 0 else seg + 1}
        ref = edge_m if kind else edge_fc
        if kind:
            src, dst = ref.at[direction, pl.ds(1, 4)], ref.at[direction + 2, pl.ds(1, 4)]
        else:
            src, dst = ref.at[direction, :, pl.ds(1, 4)], ref.at[direction + 2, :, pl.ds(1, 4)]
        return pltpu.make_async_remote_copy(
            src_ref=src, dst_ref=dst,
            send_sem=side_send.at[direction, kind], recv_sem=side_recv.at[direction, kind],
            device_id=device, device_id_type=MESH)

    def spread_heat(row):
        spread(f_rows[row], heat.at[0], at(row))

    def spread_fixed(row):
        spread(jnp.where(m_rows[row] != 0, -c_rows[row], c_rows[row]), cond, at(row))
        for v in range(NV):
            both = cond[at(row), reg(v), :]
            keep[at(row), reg(v), :] = jnp.where(both < 0.0, 0.0, 1.0)
            cond[at(row), reg(v), :] = jnp.abs(both)

    for copy in edge_loads():
        copy.wait()
    for direction, there in ((0, has_west), (1, has_east)):
        @pl.when(there)
        def _():
            side_copy(direction, 0).start()
            side_copy(direction, 1).start()
    for k in range(3):
        wait_loads(k, 0)
    for row in groups[0]:
        spread_heat(row)
        spread_fixed(row)
    send(0)
    send(1)
    for k in range(3):
        wait_loads(k, 1)

    @pl.loop(0, 2)
    def _(i):
        for j in range(3):
            spread_fixed(1 + 27 * i + j)

    send(2)
    send(3)

    zero = jnp.zeros((8, 128), jnp.float32)
    for there, first in ((has_up, -GHOST), (has_down, ROWS)):
        @pl.when(jnp.logical_not(there))
        def _():
            @pl.loop(0, GHOST)
            def _(i):
                for v in range(NV):
                    for ref in (heat.at[0], heat.at[1], cond, keep):
                        ref[at(first) + i, reg(v), :] = zero

    def east_row(row):
        c = load(cond, row)
        c.append(after_last(c[0]))
        for v in range(NV):
            face = FACE * (c[v] + c[v + 1])
            east[row, reg(v), :] = face
        west[row] = before_first(face)

    def south_row(row):
        for v in range(NV):
            south[row, reg(v), :] = FACE * (
                cond[row, reg(v), :] + cond[row + 1, reg(v), :])

    @pl.loop(0, 2)
    def _(i):
        for j in range(3):
            spread_heat(1 + 27 * i + j)

    for k in range(3):
        wait_loads(k, 2)

    @pl.loop(0, 12)
    def _(i):
        for j in range(2):
            spread_fixed(4 + 2 * i + j)
            spread_heat(4 + 2 * i + j)

    @pl.loop(0, ROWS // 4)
    def _(i):
        for j in range(4):
            east_row(at(0) + 4 * i + j)

    @pl.loop(0, ROWS // 4)
    def _(i):
        for j in range(4):
            south_row(at(0) + jnp.minimum(4 * i + j, ROWS - 2))

    def rows_step(time, rows, first=False, put=None):
        old, new = heat.at[(time - 1) % 2], heat.at[time % 2]
        above = load(old, rows[0] - 1)
        here = load(old, rows[0])
        north = [south[rows[0] - 1, reg(v), :] * (here[v] - above[v]) for v in range(NV)]
        for i, row in enumerate(rows):
            below = load(old, row + 1)
            ahead = here[1:] + [after_last(here[0])]
            behind = west[row] * (here[0] - before_first(here[-1]))
            down = []
            for v in range(NV):
                down.append(south[row, reg(v), :] * (below[v] - here[v]))
                flow = east[row, reg(v), :] * (ahead[v] - here[v])
                change = (flow - behind) + (down[v] - north[v])
                behind = flow
                if first:
                    value = jnp.where(keep[row, reg(v), :] == 0.0, 1.0, here[v] + change)
                else:
                    value = here[v] + keep[row, reg(v), :] * change
                if put is None:
                    new[row, reg(v), :] = value
                else:
                    put(i, v, value)
            here, north = below, down

    def sweep(time, low, high, width, first=False):
        count = -(-(high - low) // width)

        @pl.loop(0, count)
        def _(i):
            start = at(jnp.minimum(low + i * width, high - width))
            rows_step(time, [start + j for j in range(width)], first)

    sweep(1, 1, ROWS - 1, 6, first=True)

    for direction, there in ((0, has_east), (1, has_west)):
        @pl.when(there)
        def _():
            side_copy(direction, 0).wait_recv()
            side_copy(direction, 1).wait_recv()
    received(0)
    received(1)
    south_row(at(-1))
    south_row(at(ROWS - 1))
    rows_step(1, [at(0)], first=True)
    rows_step(1, [at(ROWS - 1)], first=True)
    send(6)
    send(7)
    send(4)
    send(5)

    for time in range(2, STEPS + 1):
        level = time - 1
        sweep(time, level, ROWS - level, 6)
        for slot, (_, when) in enumerate(LINES):
            if when == time:
                send(6 + slot)

    received(4)
    received(5)
    shape = (48, 128)
    lane48 = lax.broadcasted_iota(jnp.int32, shape, 1)
    row48 = lax.broadcasted_iota(jnp.int32, shape, 0)
    first_row = jnp.where(has_up, 0, 8)
    end_row = jnp.where(has_down, 48, 40)
    turns = ((127, 1), (1, 1), (47, 0), (1, 0))

    def substep(f, faces):
        total = f
        for turn, face in zip(turns, faces):
            total = total + face * (pltpu.roll(f, *turn) - f)
        return total

    starts, all_faces = [], []
    for side in range(2):
        right, left = ((0, 3), (2, 1))[side]
        is_right = lane48 < 64
        first_lane = 0 if side == 0 else jnp.where(has_east, 0, 64)
        end_lane = jnp.where(has_west, 128, 64) if side == 0 else 128
        exists = ((row48 >= first_row) & (row48 < end_row)
                  & (lane48 >= first_lane) & (lane48 < end_lane))

        def pick(k):
            value = jnp.where(is_right, edge_fc[right, k].reshape(shape),
                              edge_fc[left, k].reshape(shape))
            return jnp.where(exists, value, 0.0)

        f = pick(0)
        c = pick(1)
        source = jnp.where(is_right, edge_m[right].reshape(shape),
                           edge_m[left].reshape(shape)) != 0
        source = jnp.logical_and(source, exists)
        stay = jnp.where(jnp.logical_and(exists, jnp.logical_not(source)), 1.0, 0.0)
        faces = [stay * (FACE * (c + pltpu.roll(c, *turn))) for turn in turns]
        starts.append(jnp.where(source, 1.0, substep(f, faces)))
        all_faces.append(faces)

    ends = lax.fori_loop(
        1, STEPS,
        lambda _, fs: tuple(substep(f, faces) for f, faces in zip(fs, all_faces)),
        tuple(starts))
    for side in range(2):
        edge_out[side] = ends[side][8:40]

    @pl.loop(LOW, HIGH)
    def _(row):
        def put(where, value):
            ready[row, where, :] = value

        finish(heat.at[STEPS % 2], at(row), edge_out, row, put)

    received(2)
    received(3)
    for row in (-3, -2, -1, ROWS, ROWS + 1, ROWS + 2):
        east_row(at(row))

    for row in (-4, -3, -2, ROWS, ROWS + 1, ROWS + 2):
        south_row(at(row))

    for slot in range(13):
        sent(slot)
    for slot in range(6, 13):
        received(slot)
    for time in range(2, STEPS + 1):
        level = time - 1
        out_by = min(level, 7 - level)
        top = [at(row) for row in range(-out_by, level)]
        bottom = [at(row) for row in range(ROWS - level, ROWS + out_by)]
        for half, rows in enumerate((top, bottom)):
            put = None
            if time == STEPS:
                def put(i, v, value, half=half):
                    border[LOW * half + i, reg(v), :] = value
            rows_step(time, rows, put=put)
    for direction, there in ((0, has_west), (1, has_east)):
        @pl.when(there)
        def _():
            side_copy(direction, 0).wait_send()
            side_copy(direction, 1).wait_send()


def write(ready, border, edge, out, rest, sem):
    def copy(src, row, slot):
        return pltpu.make_async_copy(src, out.at[row // 8, :, row % 8], sem.at[slot])

    last = [(i, i if i < LOW else HIGH + i - LOW) for i in range(2 * LOW)]
    for row in range(LOW, HIGH):
        copy(ready.at[row], row, row).start()
    for i, row in last:
        def put(where, value):
            rest[i, where, :] = value

        finish(border, i, edge, row, put)
        copy(rest.at[i], row, row).start()
    for row in range(LOW, HIGH):
        copy(ready.at[row], row, row).wait()
    for i, row in last:
        copy(rest.at[i], row, row).wait()


def tiles(x):
    return x.reshape(4, 8, 128, 128).transpose(0, 2, 1, 3)


def shards(starting_warmth, diffusivity_field, emitter_mask):
    wide = ROWS + 2 * GHOST
    values = (128, 128)
    inside = pl.BlockSpec(memory_space=pltpu.VMEM)
    outside = pl.BlockSpec(memory_space=pltpu.HBM)
    ready, border, edge = pl.pallas_call(
        kernel,
        out_shape=(
            jax.ShapeDtypeStruct((ROWS, 128, 128), jnp.float32),
            jax.ShapeDtypeStruct((2 * LOW, *values), jnp.float32),
            jax.ShapeDtypeStruct((2, ROWS, 128), jnp.float32),
        ),
        in_specs=[outside] * 3,
        out_specs=(inside,) * 3,
        scratch_shapes=[
            pltpu.VMEM((ROWS, 128, 128), jnp.float32),
            pltpu.VMEM((ROWS, 128, 128), jnp.float32),
            pltpu.VMEM((ROWS, 128, 128), jnp.int32),
            pltpu.VMEM((2, wide, *values), jnp.float32),
            pltpu.VMEM((wide, *values), jnp.float32),
            pltpu.VMEM((wide, *values), jnp.float32),
            pltpu.VMEM((wide, 8, 128), jnp.float32),
            pltpu.VMEM((wide, *values), jnp.float32),
            pltpu.VMEM((wide, *values), jnp.float32),
            pltpu.VMEM((4, 2, 6, 8, 128), jnp.float32),
            pltpu.VMEM((4, 6, 8, 128), jnp.int32),
            pltpu.SemaphoreType.DMA((3, 3)),
            pltpu.SemaphoreType.DMA((6,)),
            pltpu.SemaphoreType.DMA((2, 13)),
            pltpu.SemaphoreType.DMA((2, 13)),
            pltpu.SemaphoreType.DMA((2, 2)),
            pltpu.SemaphoreType.DMA((2, 2)),
        ],
        compiler_params=pltpu.CompilerParams(
            collective_id=0, has_side_effects=True, vmem_limit_bytes=50 * 2**20),
    )(tiles(starting_warmth), tiles(diffusivity_field), tiles(emitter_mask))
    result = pl.pallas_call(
        write,
        out_shape=jax.ShapeDtypeStruct((4, 128, 8, 128), jnp.float32),
        in_specs=[inside] * 3,
        out_specs=outside,
        scratch_shapes=[
            pltpu.VMEM((2 * LOW, 128, 128), jnp.float32),
            pltpu.SemaphoreType.DMA((ROWS,)),
        ],
        compiler_params=pltpu.CompilerParams(vmem_limit_bytes=16 * 2**20),
    )(ready, border, edge)
    return result.transpose(0, 2, 1, 3).reshape(ROWS, 128 * 128)


def solution(mesh):
    return jax.shard_map(
        shards,
        mesh=mesh,
        in_specs=(P("tile", "seg"),) * 3,
        out_specs=P("tile", "seg"),
        check_vma=False,
    )
```

```python
import functools

import jax
import jax.numpy as jnp
from jax import lax
from jax.experimental import pallas as pl
from jax.experimental.pallas import tpu as pltpu
from jax.sharding import PartitionSpec as P

STEPS = 8
FACE = 0.24 * 0.5
ROWS = 32
GHOST = 4
NV = 16
LOW, HIGH = 7, 25
MESH = pl.DeviceIdType.MESH

LINES = ((1, 2), (2, 3), (3, 4), (4, 4))
SLOTS = 6 + len(LINES)
FILLS = (((6, 7), 1, 4), ((8,), 5, 6), ((9,), 7, 7))


def at(row):
    return row + GHOST


def reg(v):
    return pl.ds(8 * v, 8)


def load(ref, row):
    return [ref[row, reg(v), :] for v in range(NV)]


def position():
    return (lax.broadcasted_iota(jnp.int32, (8, 128), 0),
            lax.broadcasted_iota(jnp.int32, (8, 128), 1))


def after_last(first):
    sub, _ = position()
    down = pltpu.roll(first, 7, 0)
    return jnp.where(sub == 7, pltpu.roll(down, 127, 1), down)


def before_first(last):
    sub, _ = position()
    up = pltpu.roll(last, 1, 0)
    return jnp.where(sub == 0, pltpu.roll(up, 1, 1), up)


def comb(j):
    return pl.ds(64 * (j % 2) + j // 2, 8, stride=8)


def spread(x, ref, row):
    turned = x.T
    for j in range(NV):
        ref[row, comb(j), :] = turned[8 * j:8 * j + 8]


def gather(ref, row):
    return jnp.concatenate([ref[row, comb(j), :] for j in range(NV)], axis=0).T


def finish(ref, at_row, edge, row, put):
    sub, lane = position()
    x = gather(ref, at_row)
    for side, first, where in ((0, 0, (sub == 0) & (lane < 8)),
                               (1, 120, (sub == 7) & (lane >= 120))):
        patch = jnp.broadcast_to(edge[side, pl.ds(row, 1), :], (8, 128))
        put(pl.ds(first, 8), jnp.where(where, patch, x[first:first + 8]))
    put(pl.ds(8, 112), x[8:120])


def kernel(
    f_in, c_in, m_in,
    ready, border, edge_out,
    f_rows, c_rows, m_rows, heat, cond, east, west, south, keep,
    edge_fc, edge_m,
    load_sem, edge_load_sem, send_sem, recv_sem, side_send, side_recv,
):
    tile = lax.axis_index("tile")
    seg = lax.axis_index("seg")
    n_tile = lax.axis_size("tile")
    n_seg = lax.axis_size("seg")
    has_up = tile > 0
    has_down = tile < n_tile - 1
    has_west = seg > 0
    has_east = seg < n_seg - 1

    barrier = pltpu.get_barrier_semaphore()
    sides = (
        (has_up, {"tile": tile - 1}), (has_down, {"tile": tile + 1}),
        (has_west, {"seg": seg - 1}), (has_east, {"seg": seg + 1}),
    )
    for there, device in sides:
        @pl.when(there)
        def _():
            pl.semaphore_signal(barrier, inc=1, device_id=device, device_id_type=MESH)
    count = sum(there.astype(jnp.int32) for there, _ in sides)

    def edge_loads():
        copies = []
        for piece, block in enumerate((0, 127)):
            for k, src in enumerate((f_in, c_in)):
                copies.append(pltpu.make_async_copy(
                    src.at[:, block], edge_fc.at[piece, k, pl.ds(1, 4)],
                    edge_load_sem.at[3 * piece + k]))
            copies.append(pltpu.make_async_copy(
                m_in.at[:, block], edge_m.at[piece, pl.ds(1, 4)],
                edge_load_sem.at[3 * piece + 2]))
        return copies

    arrays = ((f_in, f_rows), (c_in, c_rows), (m_in, m_rows))
    groups = ((0, 31), (1, 2, 3, 28, 29, 30), tuple(range(4, 28)))

    def start_loads(k, group):
        src, dst = arrays[k]
        for row in groups[group]:
            pltpu.make_async_copy(
                src.at[row // 8, :, row % 8], dst.at[row], load_sem.at[k, group]).start()

    def wait_loads(k, group):
        dst = arrays[k][1].at[pl.ds(0, len(groups[group]))]
        pltpu.make_async_copy(dst, dst, load_sem.at[k, group]).wait()

    for k in range(3):
        start_loads(k, 0)
    for k in (1, 2):
        start_loads(k, 1)
    for copy in edge_loads():
        copy.start()

    pl.semaphore_wait(barrier, count)

    def rows_of(direction, near, far):
        if direction == 0:
            return near - 1, ROWS + near - 1, far - near + 1
        return ROWS - far, -far, far - near + 1

    def remote(direction, slot, src, dst):
        device = {"tile": tile - 1 if direction == 0 else tile + 1}
        return pltpu.make_async_remote_copy(
            src_ref=src, dst_ref=dst,
            send_sem=send_sem.at[direction, slot], recv_sem=recv_sem.at[direction, slot],
            device_id=device, device_id_type=MESH)

    def tile_copy(direction, slot):
        if slot == 0:
            ref, near, far = heat.at[0], 1, 1
        elif slot == 1:
            ref, near, far = cond, 1, 1
        elif slot == 2:
            ref, near, far = cond, 2, 4
        elif slot == 3:
            ref, near, far = keep, 1, 3
        elif slot < 6:
            block = 1 if direction == 0 else 4
            land = 5 if direction == 0 else 0
            if slot == 4:
                return remote(direction, slot, edge_fc.at[:, :, block], edge_fc.at[:, :, land])
            return remote(direction, slot, edge_m.at[:, block], edge_m.at[:, land])
        else:
            near, far = LINES[slot - 6]
            ref = heat.at[(slot - 5) % 2]
        src, dst, count = rows_of(direction, near, far)
        return remote(direction, slot, ref.at[pl.ds(at(src), count)],
                      ref.at[pl.ds(at(dst), count)])

    def send(slot):
        for direction, there in ((0, has_up), (1, has_down)):
            @pl.when(there)
            def _():
                tile_copy(direction, slot).start()

    first_core = tile % 2 == 0

    def send_far(slot):
        for direction, there in ((0, has_up), (1, has_down & jnp.logical_not(first_core))):
            @pl.when(there)
            def _():
                tile_copy(direction, slot).start()

    def send_near(slot):
        @pl.when(has_down & first_core)
        def _():
            tile_copy(1, slot).start()

    def sent(slot):
        for direction, there in ((0, has_up), (1, has_down)):
            @pl.when(there)
            def _():
                tile_copy(direction, slot).wait_send()

    def received(slot):
        for direction, there in ((0, has_down), (1, has_up)):
            @pl.when(there)
            def _():
                tile_copy(direction, slot).wait_recv()

    def side_copy(direction, kind):
        device = {"seg": seg - 1 if direction == 0 else seg + 1}
        ref = edge_m if kind else edge_fc
        if kind:
            src, dst = ref.at[direction, pl.ds(1, 4)], ref.at[direction + 2, pl.ds(1, 4)]
        else:
            src, dst = ref.at[direction, :, pl.ds(1, 4)], ref.at[direction + 2, :, pl.ds(1, 4)]
        return pltpu.make_async_remote_copy(
            src_ref=src, dst_ref=dst,
            send_sem=side_send.at[direction, kind], recv_sem=side_recv.at[direction, kind],
            device_id=device, device_id_type=MESH)

    def spread_heat(row):
        spread(f_rows[row], heat.at[0], at(row))

    def spread_fixed(row):
        spread(jnp.where(m_rows[row] != 0, -c_rows[row], c_rows[row]), cond, at(row))
        for v in range(NV):
            both = cond[at(row), reg(v), :]
            keep[at(row), reg(v), :] = jnp.where(both < 0.0, 0.0, 1.0)
            cond[at(row), reg(v), :] = jnp.abs(both)

    for k in range(3):
        wait_loads(k, 0)
    start_loads(0, 1)
    for k in (0, 1, 2):
        start_loads(k, 2)
    for row in groups[0]:
        spread_heat(row)
        spread_fixed(row)
    send(0)
    send(1)
    for copy in edge_loads():
        copy.wait()
    for direction, there in ((0, has_west), (1, has_east)):
        @pl.when(there)
        def _():
            side_copy(direction, 0).start()
            side_copy(direction, 1).start()
    for k in (1, 2):
        wait_loads(k, 1)

    @pl.loop(0, 2)
    def _(i):
        for j in range(3):
            spread_fixed(1 + 27 * i + j)

    send(2)
    send(3)

    zero = jnp.zeros((8, 128), jnp.float32)
    for there, first in ((has_up, -GHOST), (has_down, ROWS)):
        @pl.when(jnp.logical_not(there))
        def _():
            @pl.loop(0, GHOST)
            def _(i):
                for v in range(NV):
                    for ref in (heat.at[0], heat.at[1], cond, keep):
                        ref[at(first) + i, reg(v), :] = zero

    def east_row(row):
        c = load(cond, row)
        c.append(after_last(c[0]))
        for v in range(NV):
            face = FACE * (c[v] + c[v + 1])
            east[row, reg(v), :] = face
        west[row] = before_first(face)

    def south_row(row):
        for v in range(NV):
            south[row, reg(v), :] = FACE * (
                cond[row, reg(v), :] + cond[row + 1, reg(v), :])

    wait_loads(0, 1)

    @pl.loop(0, 2)
    def _(i):
        for j in range(3):
            spread_heat(1 + 27 * i + j)

    for k in range(3):
        wait_loads(k, 2)

    @pl.loop(0, 12)
    def _(i):
        for j in range(2):
            spread_fixed(4 + 2 * i + j)
            spread_heat(4 + 2 * i + j)

    def rows_step(time, rows, put=None):
        old, new = heat.at[(time - 1) % 2], heat.at[time % 2]
        above = load(old, rows[0] - 1)
        here = load(old, rows[0])
        north = [south[rows[0] - 1, reg(v), :] * (here[v] - above[v]) for v in range(NV)]
        for i, row in enumerate(rows):
            below = load(old, row + 1)
            ahead = here[1:] + [after_last(here[0])]
            behind = west[row] * (here[0] - before_first(here[-1]))
            down = []
            for v in range(NV):
                down.append(south[row, reg(v), :] * (below[v] - here[v]))
                flow = east[row, reg(v), :] * (ahead[v] - here[v])
                change = (flow - behind) + (down[v] - north[v])
                behind = flow
                value = here[v] + keep[row, reg(v), :] * change
                if put is None:
                    new[row, reg(v), :] = value
                else:
                    put(i, v, value)
            here, north = below, down

    def sweep(time, low, high, width):
        count = -(-(high - low) // width)

        @pl.loop(0, count)
        def _(i):
            start = at(jnp.minimum(low + i * width, high - width))
            rows_step(time, [start + j for j in range(width)])

    def first_step(rows):
        old, new = heat.at[0], heat.at[1]
        above, here = load(old, rows[0] - 1), load(old, rows[0])
        c_above, c = load(cond, rows[0] - 1), load(cond, rows[0])
        north = []
        for v in range(NV):
            face = FACE * (c_above[v] + c[v])
            south[rows[0] - 1, reg(v), :] = face
            north.append(face * (here[v] - above[v]))
        for row in rows:
            below, c_below = load(old, row + 1), load(cond, row + 1)
            ahead = here[1:] + [after_last(here[0])]
            c_ahead = c[1:] + [after_last(c[0])]
            face = FACE * (c[-1] + c_ahead[-1])
            west_face = before_first(face)
            west[row] = west_face
            behind = west_face * (here[0] - before_first(here[-1]))
            down = []
            for v in range(NV):
                face = FACE * (c[v] + c_below[v])
                south[row, reg(v), :] = face
                down.append(face * (below[v] - here[v]))
                face = FACE * (c[v] + c_ahead[v])
                east[row, reg(v), :] = face
                flow = face * (ahead[v] - here[v])
                change = (flow - behind) + (down[v] - north[v])
                behind = flow
                new[row, reg(v), :] = jnp.where(
                    keep[row, reg(v), :] == 0.0, 1.0, here[v] + change)
            here, north, c = below, down, c_below

    @pl.loop(0, (ROWS - 2) // 3)
    def _(i):
        first_step([at(1) + 3 * i + j for j in range(3)])

    for direction, there in ((0, has_east), (1, has_west)):
        @pl.when(there)
        def _():
            side_copy(direction, 0).wait_recv()
            side_copy(direction, 1).wait_recv()
    received(0)
    received(1)
    first_step([at(0)])
    first_step([at(ROWS - 1)])
    send_far(6)
    send(4)
    send(5)

    for time in range(2, STEPS + 1):
        level = time - 1
        sweep(time, level, ROWS - level, 6)
        if time <= len(LINES):
            send_far(5 + time)
        if time == len(LINES):
            for slot in range(6, SLOTS):
                send_near(slot)

    received(4)
    received(5)
    shape = (48, 128)
    lane48 = lax.broadcasted_iota(jnp.int32, shape, 1)
    row48 = lax.broadcasted_iota(jnp.int32, shape, 0)
    first_row = jnp.where(has_up, 0, 8)
    end_row = jnp.where(has_down, 48, 40)
    turns = ((127, 1), (1, 1), (47, 0), (1, 0))

    def substep(f, faces):
        total = f
        for turn, face in zip(turns, faces):
            total = total + face * (pltpu.roll(f, *turn) - f)
        return total

    starts, all_faces = [], []
    for side in range(2):
        right, left = ((0, 3), (2, 1))[side]
        is_right = lane48 < 64
        first_lane = 0 if side == 0 else jnp.where(has_east, 0, 64)
        end_lane = jnp.where(has_west, 128, 64) if side == 0 else 128
        exists = ((row48 >= first_row) & (row48 < end_row)
                  & (lane48 >= first_lane) & (lane48 < end_lane))

        def pick(k):
            value = jnp.where(is_right, edge_fc[right, k].reshape(shape),
                              edge_fc[left, k].reshape(shape))
            return jnp.where(exists, value, 0.0)

        f = pick(0)
        c = pick(1)
        source = jnp.where(is_right, edge_m[right].reshape(shape),
                           edge_m[left].reshape(shape)) != 0
        source = jnp.logical_and(source, exists)
        stay = jnp.where(jnp.logical_and(exists, jnp.logical_not(source)), 1.0, 0.0)
        faces = [stay * (FACE * (c + pltpu.roll(c, *turn))) for turn in turns]
        starts.append(jnp.where(source, 1.0, substep(f, faces)))
        all_faces.append(faces)

    ends = lax.fori_loop(
        1, STEPS,
        lambda _, fs: tuple(substep(f, faces) for f, faces in zip(fs, all_faces)),
        tuple(starts))
    for side in range(2):
        edge_out[side] = ends[side][8:40]

    @pl.loop(0, 3)
    def _(i):
        for j in range(6):
            row = LOW + 6 * i + j

            def put(where, value, row=row):
                ready[row, where, :] = value

            finish(heat.at[STEPS % 2], at(row), edge_out, row, put)

    received(2)
    received(3)
    for row in (-3, -2, -1, ROWS, ROWS + 1, ROWS + 2):
        east_row(at(row))

    for row in (-4, -3, -2, ROWS, ROWS + 1, ROWS + 2):
        south_row(at(row))

    for slot in range(SLOTS):
        sent(slot)
    for slots, low, high in FILLS:
        for slot in slots:
            received(slot)
        for level in range(1, STEPS):
            last = min(high, 2 * level)
            if last < low:
                continue
            top = list(range(level - last, level - low + 1))
            bottom = [ROWS - 1 - row for row in reversed(top)]
            for rows, shift in ((top, 0), (bottom, 2 * LOW - ROWS)):
                put = None
                if level == STEPS - 1:
                    def put(i, v, value, start=rows[0] + shift):
                        border[start + i, reg(v), :] = value
                rows_step(level + 1, [at(row) for row in rows], put=put)
    for direction, there in ((0, has_west), (1, has_east)):
        @pl.when(there)
        def _():
            side_copy(direction, 0).wait_send()
            side_copy(direction, 1).wait_send()


def write(ready, border, edge, out, rest, sem):
    def copy(src, row, slot):
        return pltpu.make_async_copy(src, out.at[row // 8, :, row % 8], sem.at[slot])

    last = [(i, i if i < LOW else HIGH + i - LOW) for i in range(2 * LOW)]
    for row in range(LOW, HIGH):
        copy(ready.at[row], row, row).start()
    for i, row in last:
        def put(where, value):
            rest[i, where, :] = value

        finish(border, i, edge, row, put)
        copy(rest.at[i], row, row).start()
    for row in range(LOW, HIGH):
        copy(ready.at[row], row, row).wait()
    for i, row in last:
        copy(rest.at[i], row, row).wait()


def tiles(x):
    return x.reshape(4, 8, 128, 128).transpose(0, 2, 1, 3)


def shards(starting_warmth, diffusivity_field, emitter_mask):
    wide = ROWS + 2 * GHOST
    values = (128, 128)
    inside = pl.BlockSpec(memory_space=pltpu.VMEM)
    outside = pl.BlockSpec(memory_space=pltpu.HBM)
    ready, border, edge = pl.pallas_call(
        kernel,
        out_shape=(
            jax.ShapeDtypeStruct((ROWS, 128, 128), jnp.float32),
            jax.ShapeDtypeStruct((2 * LOW, *values), jnp.float32),
            jax.ShapeDtypeStruct((2, ROWS, 128), jnp.float32),
        ),
        in_specs=[outside] * 3,
        out_specs=(inside,) * 3,
        scratch_shapes=[
            pltpu.VMEM((ROWS, 128, 128), jnp.float32),
            pltpu.VMEM((ROWS, 128, 128), jnp.float32),
            pltpu.VMEM((ROWS, 128, 128), jnp.int32),
            pltpu.VMEM((2, wide, *values), jnp.float32),
            pltpu.VMEM((wide, *values), jnp.float32),
            pltpu.VMEM((wide, *values), jnp.float32),
            pltpu.VMEM((wide, 8, 128), jnp.float32),
            pltpu.VMEM((wide, *values), jnp.float32),
            pltpu.VMEM((wide, *values), jnp.float32),
            pltpu.VMEM((4, 2, 6, 8, 128), jnp.float32),
            pltpu.VMEM((4, 6, 8, 128), jnp.int32),
            pltpu.SemaphoreType.DMA((3, 3)),
            pltpu.SemaphoreType.DMA((6,)),
            pltpu.SemaphoreType.DMA((2, SLOTS)),
            pltpu.SemaphoreType.DMA((2, SLOTS)),
            pltpu.SemaphoreType.DMA((2, 2)),
            pltpu.SemaphoreType.DMA((2, 2)),
        ],
        compiler_params=pltpu.CompilerParams(
            collective_id=0, has_side_effects=True, vmem_limit_bytes=50 * 2**20),
    )(tiles(starting_warmth), tiles(diffusivity_field), tiles(emitter_mask))
    result = pl.pallas_call(
        write,
        out_shape=jax.ShapeDtypeStruct((4, 128, 8, 128), jnp.float32),
        in_specs=[inside] * 3,
        out_specs=outside,
        scratch_shapes=[
            pltpu.VMEM((2 * LOW, 128, 128), jnp.float32),
            pltpu.SemaphoreType.DMA((ROWS,)),
        ],
        compiler_params=pltpu.CompilerParams(vmem_limit_bytes=16 * 2**20),
    )(ready, border, edge)
    return result.transpose(0, 2, 1, 3).reshape(ROWS, 128 * 128)


def solution(mesh):
    return jax.shard_map(
        shards,
        mesh=mesh,
        in_specs=(P("tile", "seg"),) * 3,
        out_specs=P("tile", "seg"),
        check_vma=False,
    )
```

```python
import functools

import jax
import jax.numpy as jnp
from jax import lax
from jax.experimental import pallas as pl
from jax.experimental.pallas import tpu as pltpu
from jax.sharding import PartitionSpec as P

STEPS = 8
FACE = 0.24 * 0.5
ROWS = 32
GHOST = 4
NV = 16
LAST = 3
LOW, HIGH = 7, 25
MESH = pl.DeviceIdType.MESH

LINES = ((1, 2), (2, 3), (3, 4), (4, 4))
SLOTS = 5 + len(LINES)
FILLS = (((5, 6), 1, 4), ((7,), 5, 6), ((8,), 7, 7))


def at(row):
    return row + GHOST


def reg(v):
    return pl.ds(8 * v, 8)


def load(ref, row):
    return [ref[row, reg(v), :] for v in range(NV)]


def position():
    return (lax.broadcasted_iota(jnp.int32, (8, 128), 0),
            lax.broadcasted_iota(jnp.int32, (8, 128), 1))


def after_last(first):
    sub, _ = position()
    down = pltpu.roll(first, 7, 0)
    return jnp.where(sub == 7, pltpu.roll(down, 127, 1), down)


def before_first(last):
    sub, _ = position()
    up = pltpu.roll(last, 1, 0)
    return jnp.where(sub == 0, pltpu.roll(up, 1, 1), up)


def comb(j):
    return pl.ds(64 * (j % 2) + j // 2, 8, stride=8)


def spread(x, ref, row):
    turned = x.T
    for j in range(NV):
        ref[row, comb(j), :] = turned[8 * j:8 * j + 8]


def gather(ref, row):
    return jnp.concatenate([ref[row, comb(j), :] for j in range(NV)], axis=0).T


def finish(ref, at_row, edge, row, put):
    sub, lane = position()
    x = gather(ref, at_row)
    for side, first, where in ((0, 0, (sub == 0) & (lane < 8)),
                               (1, 120, (sub == 7) & (lane >= 120))):
        patch = jnp.broadcast_to(edge[side, pl.ds(row, 1), :], (8, 128))
        put(pl.ds(first, 8), jnp.where(where, patch, x[first:first + 8]))
    put(pl.ds(8, 112), x[8:120])


def kernel(
    f_in, c_in, m_in,
    ready, border, edge_out,
    f_rows, c_rows, m_rows, heat, cond, east, west, south, keep,
    edge_fc, edge_m, edges,
    load_sem, edge_load_sem, send_sem, recv_sem, side_send, side_recv,
):
    tile = lax.axis_index("tile")
    seg = lax.axis_index("seg")
    n_tile = lax.axis_size("tile")
    n_seg = lax.axis_size("seg")
    has_up = tile > 0
    has_down = tile < n_tile - 1
    has_west = seg > 0
    has_east = seg < n_seg - 1

    barrier = pltpu.get_barrier_semaphore()
    sides = (
        (has_up, {"tile": tile - 1}), (has_down, {"tile": tile + 1}),
        (has_west, {"seg": seg - 1}), (has_east, {"seg": seg + 1}),
    )
    for there, device in sides:
        @pl.when(there)
        def _():
            pl.semaphore_signal(barrier, inc=1, device_id=device, device_id_type=MESH)
    count = sum(there.astype(jnp.int32) for there, _ in sides)

    def edge_loads():
        copies = []
        for piece, block in enumerate((0, 127)):
            for k, src in enumerate((f_in, c_in)):
                copies.append(pltpu.make_async_copy(
                    src.at[:, block], edge_fc.at[piece, k],
                    edge_load_sem.at[3 * piece + k]))
            copies.append(pltpu.make_async_copy(
                m_in.at[:, block], edge_m.at[piece],
                edge_load_sem.at[3 * piece + 2]))
        return copies

    arrays = ((f_in, f_rows), (c_in, c_rows), (m_in, m_rows))
    groups = ((0, 31), (1, 2, 3, 28, 29, 30), tuple(range(4, 28)))

    def start_loads(k, group):
        src, dst = arrays[k]
        for row in groups[group]:
            pltpu.make_async_copy(
                src.at[row // 8, :, row % 8], dst.at[row], load_sem.at[k, group]).start()

    def wait_loads(k, group):
        dst = arrays[k][1].at[pl.ds(0, len(groups[group]))]
        pltpu.make_async_copy(dst, dst, load_sem.at[k, group]).wait()

    for k in range(3):
        start_loads(k, 0)
    for k in (1, 2):
        start_loads(k, 1)
    for copy in edge_loads():
        copy.start()


    def rows_of(direction, near, far):
        if direction == 0:
            return near - 1, ROWS + near - 1, far - near + 1
        return ROWS - far, -far, far - near + 1

    def remote(direction, slot, src, dst):
        device = {"tile": tile - 1 if direction == 0 else tile + 1}
        return pltpu.make_async_remote_copy(
            src_ref=src, dst_ref=dst,
            send_sem=send_sem.at[direction, slot], recv_sem=recv_sem.at[direction, slot],
            device_id=device, device_id_type=MESH)

    def tile_copy(direction, slot):
        if slot == 0:
            ref, near, far = heat.at[0], 1, 1
        elif slot == 1:
            ref, near, far = cond, 1, 1
        elif slot == 2:
            ref, near, far = cond, 2, 4
        elif slot == 3:
            ref, near, far = keep, 1, 3
        elif slot == 4:
            block = 1 if direction == 0 else 4
            land = 5 if direction == 0 else 0
            return remote(direction, slot, edges.at[:, :, block], edges.at[:, :, land])
        else:
            near, far = LINES[slot - 5]
            ref = heat.at[(slot - 4) % 2]
        src, dst, count = rows_of(direction, near, far)
        return remote(direction, slot, ref.at[pl.ds(at(src), count)],
                      ref.at[pl.ds(at(dst), count)])

    def send(slot):
        for direction, there in ((0, has_up), (1, has_down)):
            @pl.when(there)
            def _():
                tile_copy(direction, slot).start()

    first_core = tile % 2 == 0

    def send_far(slot):
        for direction, there in ((0, has_up), (1, has_down & jnp.logical_not(first_core))):
            @pl.when(there)
            def _():
                tile_copy(direction, slot).start()

    def send_near(slot):
        @pl.when(has_down & first_core)
        def _():
            tile_copy(1, slot).start()

    def sent(slot):
        for direction, there in ((0, has_up), (1, has_down)):
            @pl.when(there)
            def _():
                tile_copy(direction, slot).wait_send()

    def received(slot):
        for direction, there in ((0, has_down), (1, has_up)):
            @pl.when(there)
            def _():
                tile_copy(direction, slot).wait_recv()

    def side_copy(direction, kind):
        device = {"seg": seg - 1 if direction == 0 else seg + 1}
        ref = edge_m if kind else edge_fc
        src, dst = ref.at[direction], ref.at[direction + 2]
        return pltpu.make_async_remote_copy(
            src_ref=src, dst_ref=dst,
            send_sem=side_send.at[direction, kind], recv_sem=side_recv.at[direction, kind],
            device_id=device, device_id_type=MESH)

    def spread_heat(row):
        spread(f_rows[row], heat.at[0], at(row))

    def spread_fixed(row):
        spread(jnp.where(m_rows[row] != 0, -c_rows[row], c_rows[row]), cond, at(row))
        for v in range(NV):
            both = cond[at(row), reg(v), :]
            keep[at(row), reg(v), :] = jnp.where(both < 0.0, 0.0, 1.0)
            cond[at(row), reg(v), :] = jnp.abs(both)

    for k in range(3):
        wait_loads(k, 0)
    start_loads(0, 1)
    for k in (0, 1, 2):
        start_loads(k, 2)
    for row in groups[0]:
        spread_heat(row)
        spread_fixed(row)
    pl.semaphore_wait(barrier, count)
    send(0)
    send(1)
    for copy in edge_loads():
        copy.wait()
    for direction, there in ((0, has_west), (1, has_east)):
        @pl.when(there)
        def _():
            side_copy(direction, 0).start()
            side_copy(direction, 1).start()
    for k in (1, 2):
        wait_loads(k, 1)

    @pl.loop(0, 2)
    def _(i):
        for j in range(3):
            spread_fixed(1 + 27 * i + j)

    send_far(2)
    send_far(3)

    zero = jnp.zeros((8, 128), jnp.float32)
    for there, first in ((has_up, -GHOST), (has_down, ROWS)):
        @pl.when(jnp.logical_not(there))
        def _():
            @pl.loop(0, GHOST)
            def _(i):
                for v in range(NV):
                    for ref in (heat.at[0], heat.at[1], cond, keep):
                        ref[at(first) + i, reg(v), :] = zero

    def east_row(row):
        c = load(cond, row)
        c.append(after_last(c[0]))
        for v in range(NV):
            face = FACE * (c[v] + c[v + 1])
            east[row, reg(v), :] = face
        west[row] = before_first(face)

    def south_row(row):
        for v in range(NV):
            south[row, reg(v), :] = FACE * (
                cond[row, reg(v), :] + cond[row + 1, reg(v), :])

    wait_loads(0, 1)

    @pl.loop(0, 2)
    def _(i):
        for j in range(3):
            spread_heat(1 + 27 * i + j)

    for k in range(3):
        wait_loads(k, 2)

    @pl.loop(0, 12)
    def _(i):
        for j in range(2):
            spread_fixed(4 + 2 * i + j)
            spread_heat(4 + 2 * i + j)

    def rows_step(time, rows, put=None):
        old, new = heat.at[(time - 1) % 2], heat.at[time % 2]
        above = load(old, rows[0] - 1)
        here = load(old, rows[0])
        north = [south[rows[0] - 1, reg(v), :] * (here[v] - above[v]) for v in range(NV)]
        for i, row in enumerate(rows):
            below = load(old, row + 1)
            ahead = here[1:] + [after_last(here[0])]
            behind = west[row] * (here[0] - before_first(here[-1]))
            down = []
            for v in range(NV):
                down.append(south[row, reg(v), :] * (below[v] - here[v]))
                flow = east[row, reg(v), :] * (ahead[v] - here[v])
                change = (flow - behind) + (down[v] - north[v])
                behind = flow
                value = here[v] + keep[row, reg(v), :] * change
                if put is None:
                    new[row, reg(v), :] = value
                else:
                    put(i, v, value)
            here, north = below, down

    def sweep(time, low, high, width):
        count = -(-(high - low) // width)

        @pl.loop(0, count)
        def _(i):
            start = at(jnp.minimum(low + i * width, high - width))
            rows_step(time, [start + j for j in range(width)])

    def first_step(rows):
        old, new = heat.at[0], heat.at[1]
        above, here = load(old, rows[0] - 1), load(old, rows[0])
        c_above, c = load(cond, rows[0] - 1), load(cond, rows[0])
        north = []
        for v in range(NV):
            face = FACE * (c_above[v] + c[v])
            south[rows[0] - 1, reg(v), :] = face
            north.append(face * (here[v] - above[v]))
        for row in rows:
            below, c_below = load(old, row + 1), load(cond, row + 1)
            ahead = here[1:] + [after_last(here[0])]
            c_ahead = c[1:] + [after_last(c[0])]
            face = FACE * (c[-1] + c_ahead[-1])
            west_face = before_first(face)
            west[row] = west_face
            behind = west_face * (here[0] - before_first(here[-1]))
            down = []
            for v in range(NV):
                face = FACE * (c[v] + c_below[v])
                south[row, reg(v), :] = face
                down.append(face * (below[v] - here[v]))
                face = FACE * (c[v] + c_ahead[v])
                east[row, reg(v), :] = face
                flow = face * (ahead[v] - here[v])
                change = (flow - behind) + (down[v] - north[v])
                behind = flow
                new[row, reg(v), :] = jnp.where(
                    keep[row, reg(v), :] == 0.0, 1.0, here[v] + change)
            here, north, c = below, down, c_below

    @pl.loop(0, (ROWS - 2) // 3)
    def _(i):
        first_step([at(1) + 3 * i + j for j in range(3)])

    for direction, there in ((0, has_east), (1, has_west)):
        @pl.when(there)
        def _():
            side_copy(direction, 0).wait_recv()
            side_copy(direction, 1).wait_recv()
    is_right = position()[1] < 64
    for side, (right, left) in enumerate(((0, 3), (2, 1))):
        for i in range(4):
            for k in range(2):
                edges[side, k, 1 + i] = jnp.where(
                    is_right, edge_fc[right, k, i], edge_fc[left, k, i])
            marks = jnp.where(is_right, edge_m[right, i], edge_m[left, i])
            edges[side, 2, 1 + i] = jnp.where(marks != 0, 1.0, 0.0)
    send(4)
    received(0)
    received(1)
    first_step([at(0)])
    first_step([at(ROWS - 1)])
    send_far(5)

    for time in range(2, STEPS + 1):
        level = time - 1
        sweep(time, level, ROWS - level, {2: 7, 3: 7, 6: 5}.get(level, 6))
        if time <= len(LINES):
            send_far(4 + time)
        if time == len(LINES):
            for slot in (2, 3, *range(5, SLOTS)):
                send_near(slot)

    received(4)
    shape = (48, 128)
    lane48 = lax.broadcasted_iota(jnp.int32, shape, 1)
    row48 = lax.broadcasted_iota(jnp.int32, shape, 0)
    first_row = jnp.where(has_up, 0, 8)
    end_row = jnp.where(has_down, 48, 40)
    turns = ((127, 1), (1, 1), (47, 0), (1, 0))

    def substep(f, faces):
        total = f
        for turn, face in zip(turns, faces):
            total = total + face * (pltpu.roll(f, *turn) - f)
        return total

    starts, all_faces = [], []
    for side in range(2):
        first_lane = 0 if side == 0 else jnp.where(has_east, 0, 64)
        end_lane = jnp.where(has_west, 128, 64) if side == 0 else 128
        exists = ((row48 >= first_row) & (row48 < end_row)
                  & (lane48 >= first_lane) & (lane48 < end_lane))

        def pick(k):
            return jnp.where(exists, edges[side, k].reshape(shape), 0.0)

        f = pick(0)
        c = pick(1)
        source = pick(2) > 0.5
        stay = jnp.where(jnp.logical_and(exists, jnp.logical_not(source)), 1.0, 0.0)
        faces = [stay * (FACE * (c + pltpu.roll(c, *turn))) for turn in turns]
        starts.append(jnp.where(source, 1.0, substep(f, faces)))
        all_faces.append(faces)

    ends = lax.fori_loop(
        1, STEPS,
        lambda _, fs: tuple(substep(f, faces) for f, faces in zip(fs, all_faces)),
        tuple(starts))
    for side in range(2):
        edge_out[side] = ends[side][8:40]

    def in_order(first, count):
        for row in [first + j for j in range(count)]:
            def put(where, value, row=row):
                ready[row, where, :] = value

            finish(heat.at[STEPS % 2], at(row), edge_out, row, put)

    @pl.loop(0, 3)
    def _(i):
        in_order(LOW + 6 * i, 6)

    received(2)
    received(3)
    for row in (-3, -2, -1, ROWS, ROWS + 1, ROWS + 2):
        east_row(at(row))

    for row in (-4, -3, -2, ROWS, ROWS + 1, ROWS + 2):
        south_row(at(row))

    for slot in range(SLOTS):
        sent(slot)
    for slots, low, high in FILLS:
        for slot in slots:
            received(slot)
        for level in range(1, STEPS):
            last = min(high, 2 * level)
            if last < low:
                continue
            top = list(range(level - last, level - low + 1))
            bottom = [ROWS - 1 - row for row in reversed(top)]
            for rows, shift in ((top, 0), (bottom, 2 * LAST - ROWS)):
                put = None
                if level == STEPS - 1 and low > 1:
                    def put(i, v, value, start=rows[0] + shift):
                        border[start + i, reg(v), :] = value
                rows_step(level + 1, [at(row) for row in rows], put=put)
        if low == 1:
            in_order(LAST, LOW - LAST)
            in_order(HIGH, LOW - LAST)
    for direction, there in ((0, has_west), (1, has_east)):
        @pl.when(there)
        def _():
            side_copy(direction, 0).wait_send()
            side_copy(direction, 1).wait_send()


def write(ready, border, edge, out, rest, sem):
    def copy(src, row, slot):
        return pltpu.make_async_copy(src, out.at[row // 8, :, row % 8], sem.at[slot])

    last = [(i, i if i < LAST else ROWS - 2 * LAST + i) for i in range(2 * LAST)]
    for row in range(LAST, ROWS - LAST):
        copy(ready.at[row], row, row).start()
    for i, row in last:
        def put(where, value):
            rest[i, where, :] = value

        finish(border, i, edge, row, put)
        copy(rest.at[i], row, row).start()
    for row in range(LAST, ROWS - LAST):
        copy(ready.at[row], row, row).wait()
    for i, row in last:
        copy(rest.at[i], row, row).wait()


def tiles(x):
    return x.reshape(4, 8, 128, 128).transpose(0, 2, 1, 3)


def shards(starting_warmth, diffusivity_field, emitter_mask):
    wide = ROWS + 2 * GHOST
    values = (128, 128)
    inside = pl.BlockSpec(memory_space=pltpu.VMEM)
    outside = pl.BlockSpec(memory_space=pltpu.HBM)
    ready, border, edge = pl.pallas_call(
        kernel,
        out_shape=(
            jax.ShapeDtypeStruct((ROWS, 128, 128), jnp.float32),
            jax.ShapeDtypeStruct((2 * LAST, *values), jnp.float32),
            jax.ShapeDtypeStruct((2, ROWS, 128), jnp.float32),
        ),
        in_specs=[outside] * 3,
        out_specs=(inside,) * 3,
        scratch_shapes=[
            pltpu.VMEM((ROWS, 128, 128), jnp.float32),
            pltpu.VMEM((ROWS, 128, 128), jnp.float32),
            pltpu.VMEM((ROWS, 128, 128), jnp.int32),
            pltpu.VMEM((2, wide, *values), jnp.float32),
            pltpu.VMEM((wide, *values), jnp.float32),
            pltpu.VMEM((wide, *values), jnp.float32),
            pltpu.VMEM((wide, 8, 128), jnp.float32),
            pltpu.VMEM((wide, *values), jnp.float32),
            pltpu.VMEM((wide, *values), jnp.float32),
            pltpu.VMEM((4, 2, 4, 8, 128), jnp.float32),
            pltpu.VMEM((4, 4, 8, 128), jnp.int32),
            pltpu.VMEM((2, 3, 6, 8, 128), jnp.float32),
            pltpu.SemaphoreType.DMA((3, 3)),
            pltpu.SemaphoreType.DMA((6,)),
            pltpu.SemaphoreType.DMA((2, SLOTS)),
            pltpu.SemaphoreType.DMA((2, SLOTS)),
            pltpu.SemaphoreType.DMA((2, 2)),
            pltpu.SemaphoreType.DMA((2, 2)),
        ],
        compiler_params=pltpu.CompilerParams(
            collective_id=0, has_side_effects=True, vmem_limit_bytes=50 * 2**20),
    )(tiles(starting_warmth), tiles(diffusivity_field), tiles(emitter_mask))
    result = pl.pallas_call(
        write,
        out_shape=jax.ShapeDtypeStruct((4, 128, 8, 128), jnp.float32),
        in_specs=[inside] * 3,
        out_specs=outside,
        scratch_shapes=[
            pltpu.VMEM((2 * LAST, 128, 128), jnp.float32),
            pltpu.SemaphoreType.DMA((ROWS,)),
        ],
        compiler_params=pltpu.CompilerParams(vmem_limit_bytes=16 * 2**20),
    )(ready, border, edge)
    return result.transpose(0, 2, 1, 3).reshape(ROWS, 128 * 128)


def solution(mesh):
    return jax.shard_map(
        shards,
        mesh=mesh,
        in_specs=(P("tile", "seg"),) * 3,
        out_specs=P("tile", "seg"),
        check_vma=False,
    )
```

```python
import functools

import jax
import jax.numpy as jnp
from jax import lax
from jax.experimental import pallas as pl
from jax.experimental.pallas import tpu as pltpu
from jax.sharding import PartitionSpec as P

STEPS = 8
FACE = 0.24 * 0.5
ROWS = 32
GHOST = 4
NV = 16
LAST = 3
LOW, HIGH = 7, 25
MESH = pl.DeviceIdType.MESH

LINES = ((1, 2), (2, 3), (3, 4), (4, 4))
SLOTS = 5 + len(LINES)
FILLS = ((5, 1, 2), (6, 3, 4), (7, 5, 6), (8, 7, 7))


def at(row):
    return row + GHOST


def reg(v):
    return pl.ds(8 * v, 8)


def load(ref, row):
    return [ref[row, reg(v), :] for v in range(NV)]


def position():
    return (lax.broadcasted_iota(jnp.int32, (8, 128), 0),
            lax.broadcasted_iota(jnp.int32, (8, 128), 1))


def after_last(first):
    sub, _ = position()
    down = pltpu.roll(first, 7, 0)
    return jnp.where(sub == 7, pltpu.roll(down, 127, 1), down)


def before_first(last):
    sub, _ = position()
    up = pltpu.roll(last, 1, 0)
    return jnp.where(sub == 0, pltpu.roll(up, 1, 1), up)


def comb(j):
    return pl.ds(64 * (j % 2) + j // 2, 8, stride=8)


def spread(x, ref, row):
    turned = x.T
    for j in range(NV):
        ref[row, comb(j), :] = turned[8 * j:8 * j + 8]


def gather(ref, row):
    return jnp.concatenate([ref[row, comb(j), :] for j in range(NV)], axis=0).T


def finish(ref, at_row, edge, row, put):
    sub, lane = position()
    x = gather(ref, at_row)
    for j in range(NV):
        part = x[8 * j:8 * j + 8]
        for side, at_end, where in ((0, 0, (sub == 0) & (lane < 8)),
                                    (1, NV - 1, (sub == 7) & (lane >= 120))):
            if j == at_end:
                patch = jnp.broadcast_to(edge[side, pl.ds(row, 1), :], (8, 128))
                part = jnp.where(where, patch, part)
        put(j, part)


def kernel(
    f_in, c_in, m_in,
    ready, border, edge_out,
    f_rows, c_rows, m_rows, heat, cond, east, west, south, keep,
    edge_fc, edge_m, edges,
    load_sem, edge_load_sem, send_sem, recv_sem, side_send, side_recv,
):
    tile = lax.axis_index("tile")
    seg = lax.axis_index("seg")
    n_tile = lax.axis_size("tile")
    n_seg = lax.axis_size("seg")
    has_up = tile > 0
    has_down = tile < n_tile - 1
    has_west = seg > 0
    has_east = seg < n_seg - 1

    barrier = pltpu.get_barrier_semaphore()
    sides = (
        (has_up, {"tile": tile - 1}), (has_down, {"tile": tile + 1}),
        (has_west, {"seg": seg - 1}), (has_east, {"seg": seg + 1}),
    )
    for there, device in sides:
        @pl.when(there)
        def _():
            pl.semaphore_signal(barrier, inc=1, device_id=device, device_id_type=MESH)
    count = sum(there.astype(jnp.int32) for there, _ in sides)

    def edge_loads():
        copies = []
        for piece, block in enumerate((0, 127)):
            for k, src in enumerate((f_in, c_in)):
                copies.append(pltpu.make_async_copy(
                    src.at[:, block], edge_fc.at[piece, k],
                    edge_load_sem.at[3 * piece + k]))
            copies.append(pltpu.make_async_copy(
                m_in.at[:, block], edge_m.at[piece],
                edge_load_sem.at[3 * piece + 2]))
        return copies

    arrays = ((f_in, f_rows), (c_in, c_rows), (m_in, m_rows))
    groups = ((0, 31), (1, 2, 3, 28, 29, 30), tuple(range(4, 28)))

    def start_loads(k, group):
        src, dst = arrays[k]
        for row in groups[group]:
            pltpu.make_async_copy(
                src.at[row // 8, :, row % 8], dst.at[row], load_sem.at[k, group]).start()

    def wait_loads(k, group):
        dst = arrays[k][1].at[pl.ds(0, len(groups[group]))]
        pltpu.make_async_copy(dst, dst, load_sem.at[k, group]).wait()

    for k in range(3):
        start_loads(k, 0)
    for k in (1, 2):
        start_loads(k, 1)
    for copy in edge_loads():
        copy.start()


    def rows_of(direction, near, far):
        if direction == 0:
            return near - 1, ROWS + near - 1, far - near + 1
        return ROWS - far, -far, far - near + 1

    def remote(direction, slot, src, dst):
        device = {"tile": tile - 1 if direction == 0 else tile + 1}
        return pltpu.make_async_remote_copy(
            src_ref=src, dst_ref=dst,
            send_sem=send_sem.at[direction, slot], recv_sem=recv_sem.at[direction, slot],
            device_id=device, device_id_type=MESH)

    def tile_copy(direction, slot):
        if slot == 0:
            ref, near, far = heat.at[0], 1, 1
        elif slot == 1:
            ref, near, far = cond, 1, 1
        elif slot == 2:
            ref, near, far = cond, 2, 4
        elif slot == 3:
            ref, near, far = keep, 1, 3
        elif slot == 4:
            block = 1 if direction == 0 else 4
            land = 5 if direction == 0 else 0
            return remote(direction, slot, edges.at[:, :, block], edges.at[:, :, land])
        else:
            near, far = LINES[slot - 5]
            ref = heat.at[(slot - 4) % 2]
        src, dst, count = rows_of(direction, near, far)
        return remote(direction, slot, ref.at[pl.ds(at(src), count)],
                      ref.at[pl.ds(at(dst), count)])

    def send(slot):
        for direction, there in ((0, has_up), (1, has_down)):
            @pl.when(there)
            def _():
                tile_copy(direction, slot).start()

    first_core = tile % 2 == 0

    def send_far(slot):
        for direction, there in ((0, has_up), (1, has_down & jnp.logical_not(first_core))):
            @pl.when(there)
            def _():
                tile_copy(direction, slot).start()

    def send_near(slot):
        @pl.when(has_down & first_core)
        def _():
            tile_copy(1, slot).start()

    def sent(slot):
        for direction, there in ((0, has_up), (1, has_down)):
            @pl.when(there)
            def _():
                tile_copy(direction, slot).wait_send()

    def received(slot):
        for direction, there in ((0, has_down), (1, has_up)):
            @pl.when(there)
            def _():
                tile_copy(direction, slot).wait_recv()

    def side_copy(direction, kind):
        device = {"seg": seg - 1 if direction == 0 else seg + 1}
        ref = edge_m if kind else edge_fc
        src, dst = ref.at[direction], ref.at[direction + 2]
        return pltpu.make_async_remote_copy(
            src_ref=src, dst_ref=dst,
            send_sem=side_send.at[direction, kind], recv_sem=side_recv.at[direction, kind],
            device_id=device, device_id_type=MESH)

    def spread_heat(row):
        spread(f_rows[row], heat.at[0], at(row))

    def spread_fixed(row):
        spread(jnp.where(m_rows[row] != 0, -c_rows[row], c_rows[row]), cond, at(row))
        for v in range(NV):
            both = cond[at(row), reg(v), :]
            keep[at(row), reg(v), :] = jnp.where(both < 0.0, 0.0, 1.0)
            cond[at(row), reg(v), :] = jnp.abs(both)

    for k in range(3):
        wait_loads(k, 0)
    start_loads(0, 1)
    for k in (0, 1, 2):
        start_loads(k, 2)
    for row in groups[0]:
        spread_heat(row)
        spread_fixed(row)
    pl.semaphore_wait(barrier, count)
    send_far(0)
    send_far(1)
    send_near(0)
    send_near(1)
    for copy in edge_loads():
        copy.wait()
    for direction, there in ((0, has_west), (1, has_east)):
        @pl.when(there)
        def _():
            side_copy(direction, 0).start()
            side_copy(direction, 1).start()
    for k in (1, 2):
        wait_loads(k, 1)

    @pl.loop(0, 2)
    def _(i):
        for j in range(3):
            spread_fixed(1 + 27 * i + j)

    send_far(2)
    send_far(3)

    zero = jnp.zeros((8, 128), jnp.float32)
    for there, first in ((has_up, -GHOST), (has_down, ROWS)):
        @pl.when(jnp.logical_not(there))
        def _():
            @pl.loop(0, GHOST)
            def _(i):
                for v in range(NV):
                    for ref in (heat.at[0], heat.at[1], cond, keep):
                        ref[at(first) + i, reg(v), :] = zero

    def east_row(row):
        c = load(cond, row)
        c.append(after_last(c[0]))
        for v in range(NV):
            face = FACE * (c[v] + c[v + 1])
            east[row, reg(v), :] = face
        west[row] = before_first(face)

    def south_row(row):
        for v in range(NV):
            south[row, reg(v), :] = FACE * (
                cond[row, reg(v), :] + cond[row + 1, reg(v), :])

    wait_loads(0, 1)

    @pl.loop(0, 2)
    def _(i):
        for j in range(3):
            spread_heat(1 + 27 * i + j)

    for k in range(3):
        wait_loads(k, 2)

    @pl.loop(0, 12)
    def _(i):
        for j in range(2):
            spread_fixed(4 + 2 * i + j)
            spread_heat(4 + 2 * i + j)

    def rows_step(time, rows, put=None):
        old, new = heat.at[(time - 1) % 2], heat.at[time % 2]
        above = load(old, rows[0] - 1)
        here = load(old, rows[0])
        north = [south[rows[0] - 1, reg(v), :] * (here[v] - above[v]) for v in range(NV)]
        for i, row in enumerate(rows):
            below = load(old, row + 1)
            ahead = here[1:] + [after_last(here[0])]
            behind = west[row] * (here[0] - before_first(here[-1]))
            down = []
            for v in range(NV):
                down.append(south[row, reg(v), :] * (below[v] - here[v]))
                flow = east[row, reg(v), :] * (ahead[v] - here[v])
                change = (flow - behind) + (down[v] - north[v])
                behind = flow
                value = here[v] + keep[row, reg(v), :] * change
                if put is None:
                    new[row, reg(v), :] = value
                else:
                    put(i, v, value)
            here, north = below, down

    def sweep(time, low, high, width):
        count = -(-(high - low) // width)

        @pl.loop(0, count)
        def _(i):
            start = at(jnp.minimum(low + i * width, high - width))
            rows_step(time, [start + j for j in range(width)])

    def first_step(rows):
        old, new = heat.at[0], heat.at[1]
        above, here = load(old, rows[0] - 1), load(old, rows[0])
        c_above, c = load(cond, rows[0] - 1), load(cond, rows[0])
        north = []
        for v in range(NV):
            face = FACE * (c_above[v] + c[v])
            south[rows[0] - 1, reg(v), :] = face
            north.append(face * (here[v] - above[v]))
        for row in rows:
            below, c_below = load(old, row + 1), load(cond, row + 1)
            ahead = here[1:] + [after_last(here[0])]
            c_ahead = c[1:] + [after_last(c[0])]
            face = FACE * (c[-1] + c_ahead[-1])
            west_face = before_first(face)
            west[row] = west_face
            behind = west_face * (here[0] - before_first(here[-1]))
            down = []
            for v in range(NV):
                face = FACE * (c[v] + c_below[v])
                south[row, reg(v), :] = face
                down.append(face * (below[v] - here[v]))
                face = FACE * (c[v] + c_ahead[v])
                east[row, reg(v), :] = face
                flow = face * (ahead[v] - here[v])
                change = (flow - behind) + (down[v] - north[v])
                behind = flow
                new[row, reg(v), :] = jnp.where(
                    keep[row, reg(v), :] == 0.0, 1.0, here[v] + change)
            here, north, c = below, down, c_below

    @pl.loop(0, (ROWS - 2) // 3)
    def _(i):
        first_step([at(1) + 3 * i + j for j in range(3)])

    for direction, there in ((0, has_east), (1, has_west)):
        @pl.when(there)
        def _():
            side_copy(direction, 0).wait_recv()
            side_copy(direction, 1).wait_recv()
    is_right = position()[1] < 64
    for side, (right, left) in enumerate(((0, 3), (2, 1))):
        for i in range(4):
            for k in range(2):
                edges[side, k, 1 + i] = jnp.where(
                    is_right, edge_fc[right, k, i], edge_fc[left, k, i])
            marks = jnp.where(is_right, edge_m[right, i], edge_m[left, i])
            edges[side, 2, 1 + i] = jnp.where(marks != 0, 1.0, 0.0)
    send(4)
    received(0)
    received(1)
    first_step([at(0)])
    first_step([at(ROWS - 1)])
    send_far(5)

    for time in range(2, STEPS + 1):
        level = time - 1
        sweep(time, level, ROWS - level, {2: 7, 3: 7, 6: 5}.get(level, 6))
        if time <= len(LINES):
            send_far(4 + time)
        if time == len(LINES):
            for slot in (2, 3, *range(5, SLOTS)):
                send_near(slot)

    received(4)
    shape = (48, 128)
    lane48 = lax.broadcasted_iota(jnp.int32, shape, 1)
    row48 = lax.broadcasted_iota(jnp.int32, shape, 0)
    first_row = jnp.where(has_up, 0, 8)
    end_row = jnp.where(has_down, 48, 40)
    turns = ((127, 1), (1, 1), (47, 0), (1, 0))

    def substep(f, faces):
        total = f
        for turn, face in zip(turns, faces):
            total = total + face * (pltpu.roll(f, *turn) - f)
        return total

    starts, all_faces = [], []
    for side in range(2):
        first_lane = 0 if side == 0 else jnp.where(has_east, 0, 64)
        end_lane = jnp.where(has_west, 128, 64) if side == 0 else 128
        exists = ((row48 >= first_row) & (row48 < end_row)
                  & (lane48 >= first_lane) & (lane48 < end_lane))

        def pick(k):
            return jnp.where(exists, edges[side, k].reshape(shape), 0.0)

        f = pick(0)
        c = pick(1)
        source = pick(2) > 0.5
        stay = jnp.where(jnp.logical_and(exists, jnp.logical_not(source)), 1.0, 0.0)
        faces = [stay * (FACE * (c + pltpu.roll(c, *turn))) for turn in turns]
        starts.append(jnp.where(source, 1.0, substep(f, faces)))
        all_faces.append(faces)

    ends = lax.fori_loop(
        1, STEPS,
        lambda _, fs: tuple(substep(f, faces) for f, faces in zip(fs, all_faces)),
        tuple(starts))
    for side in range(2):
        edge_out[side] = ends[side][8:40]

    def in_order(first, count):
        for row in [first + j for j in range(count)]:
            def put(j, value, row=row):
                ready.reshape(4, 1024, 128)[
                    row // 8, pl.ds(64 * j + row % 8, 8, stride=8), :] = value

            finish(heat.at[STEPS % 2], at(row), edge_out, row, put)

    @pl.loop(0, 3)
    def _(i):
        in_order(LOW + 6 * i, 6)

    received(2)
    received(3)
    for row in (-3, -2, -1, ROWS, ROWS + 1, ROWS + 2):
        east_row(at(row))

    for row in (-4, -3, -2, ROWS, ROWS + 1, ROWS + 2):
        south_row(at(row))

    for slot in range(SLOTS):
        sent(slot)
    for slot, low, high in FILLS:
        received(slot)
        for level in range(1, STEPS):
            last = min(high, 2 * level)
            if last < low:
                continue
            top = list(range(level - last, level - low + 1))
            bottom = [ROWS - 1 - row for row in reversed(top)]
            for rows, shift in ((top, 0), (bottom, 2 * LAST - ROWS)):
                put = None
                if level == STEPS - 1 and high > LOW - LAST:
                    def put(i, v, value, start=rows[0] + shift):
                        border[start + i, reg(v), :] = value
                rows_step(level + 1, [at(row) for row in rows], put=put)
        if high == LOW - LAST:
            in_order(LAST, LOW - LAST)
            in_order(HIGH, LOW - LAST)
    for direction, there in ((0, has_west), (1, has_east)):
        @pl.when(there)
        def _():
            side_copy(direction, 0).wait_send()
            side_copy(direction, 1).wait_send()


def write(ready, border, edge, out, rest, sem):
    last = [(i, i if i < LAST else ROWS - 2 * LAST + i) for i in range(2 * LAST)]
    parts = [(0, LAST, 8 - LAST), (3, 0, 8 - LAST), (1, 0, 8), (2, 0, 8)]
    copies = []
    for block, first, count in parts:
        for i in range(4):
            piece = (block, pl.ds(32 * i, 32), pl.ds(first, count))
            copies.append(pltpu.make_async_copy(
                ready.at[piece], out.at[piece], sem.at[len(copies)]))
            copies[-1].start()
    for i, row in last:
        def put(j, value):
            rest[i, pl.ds(8 * j, 8), :] = value

        finish(border, i, edge, row, put)
        copies.append(pltpu.make_async_copy(
            rest.at[i], out.at[row // 8, :, row % 8], sem.at[len(copies)]))
        copies[-1].start()
    for copy in copies:
        copy.wait()


def tiles(x):
    return x.reshape(4, 8, 128, 128).transpose(0, 2, 1, 3)


def shards(starting_warmth, diffusivity_field, emitter_mask):
    wide = ROWS + 2 * GHOST
    values = (128, 128)
    inside = pl.BlockSpec(memory_space=pltpu.VMEM)
    outside = pl.BlockSpec(memory_space=pltpu.HBM)
    ready, border, edge = pl.pallas_call(
        kernel,
        out_shape=(
            jax.ShapeDtypeStruct((4, 128, 8, 128), jnp.float32),
            jax.ShapeDtypeStruct((2 * LAST, *values), jnp.float32),
            jax.ShapeDtypeStruct((2, ROWS, 128), jnp.float32),
        ),
        in_specs=[outside] * 3,
        out_specs=(inside,) * 3,
        scratch_shapes=[
            pltpu.VMEM((ROWS, 128, 128), jnp.float32),
            pltpu.VMEM((ROWS, 128, 128), jnp.float32),
            pltpu.VMEM((ROWS, 128, 128), jnp.int32),
            pltpu.VMEM((2, wide, *values), jnp.float32),
            pltpu.VMEM((wide, *values), jnp.float32),
            pltpu.VMEM((wide, *values), jnp.float32),
            pltpu.VMEM((wide, 8, 128), jnp.float32),
            pltpu.VMEM((wide, *values), jnp.float32),
            pltpu.VMEM((wide, *values), jnp.float32),
            pltpu.VMEM((4, 2, 4, 8, 128), jnp.float32),
            pltpu.VMEM((4, 4, 8, 128), jnp.int32),
            pltpu.VMEM((2, 3, 6, 8, 128), jnp.float32),
            pltpu.SemaphoreType.DMA((3, 3)),
            pltpu.SemaphoreType.DMA((6,)),
            pltpu.SemaphoreType.DMA((2, SLOTS)),
            pltpu.SemaphoreType.DMA((2, SLOTS)),
            pltpu.SemaphoreType.DMA((2, 2)),
            pltpu.SemaphoreType.DMA((2, 2)),
        ],
        compiler_params=pltpu.CompilerParams(
            collective_id=0, has_side_effects=True, vmem_limit_bytes=50 * 2**20),
    )(tiles(starting_warmth), tiles(diffusivity_field), tiles(emitter_mask))
    result = pl.pallas_call(
        write,
        out_shape=jax.ShapeDtypeStruct((4, 128, 8, 128), jnp.float32),
        in_specs=[inside] * 3,
        out_specs=outside,
        scratch_shapes=[
            pltpu.VMEM((2 * LAST, 128, 128), jnp.float32),
            pltpu.SemaphoreType.DMA((ROWS,)),
        ],
        compiler_params=pltpu.CompilerParams(vmem_limit_bytes=16 * 2**20),
    )(ready, border, edge)
    return result.transpose(0, 2, 1, 3).reshape(ROWS, 128 * 128)


def solution(mesh):
    return jax.shard_map(
        shards,
        mesh=mesh,
        in_specs=(P("tile", "seg"),) * 3,
        out_specs=P("tile", "seg"),
        check_vma=False,
    )
```
